32 devices in a mesh: tp: 4 (over z), cp: 8 (over y, x, core).
Axes of the slice: x: 2, y: 2, z: 4, core: 2. Of those that a mesh axis runs over, the one named last changes fastest.
Arguments:
- x_in: bfloat16 [1, 3072, 5120], P(None, 'cp')
- positions: int32 [3072], P('cp')
- rope_cos: float32 [3072, 128], P('cp')
- rope_sin: float32 [3072, 128], P('cp')
- norm_a: bfloat16 [5120], replicated
- wq_a: bfloat16 [5120, 5120], P(None, 'tp')
- wk_a: bfloat16 [5120, 1024], P(None, 'tp')
- wv_a: bfloat16 [5120, 1024], P(None, 'tp')
- wo_a: bfloat16 [5120, 5120], P('tp')
- norm_b: bfloat16 [5120], replicated
- wq_b: bfloat16 [5120, 5120], P(None, 'tp')
- wk_b: bfloat16 [5120, 1024], P(None, 'tp')
- wv_b: bfloat16 [5120, 1024], P(None, 'tp')
- wo_b: bfloat16 [5120, 5120], P('tp')
- grad_y: bfloat16 [1, 3072, 5120], P(None, 'cp')
Outputs:
- output 1: bfloat16 [1, 3072, 5120], P(None, 'cp')
- output 2: bfloat16 [1, 3072, 5120], P(None, 'cp')
- output 3: bfloat16 [5120], P('cp')
- output 4: bfloat16 [5120, 5120], P('cp', 'tp')
- output 5: bfloat16 [5120, 1024], P('cp', 'tp')
- output 6: bfloat16 [5120, 1024], P('cp', 'tp')
- output 7: bfloat16 [5120, 5120], P(('tp', 'cp'))
- output 8: bfloat16 [5120], P('cp')
- output 9: bfloat16 [5120, 5120], P('cp', 'tp')
- output 10: bfloat16 [5120, 1024], P('cp', 'tp')
- output 11: bfloat16 [5120, 1024], P('cp', 'tp')
- output 12: bfloat16 [5120, 5120], P(('tp', 'cp'))
All inputs are finite; a program needn't handle non-finite values.
Results may differ from the reference program's by a relative error of at most 0.02.
Values are sent between devices in bfloat16 or wider.
A program may use at most 1 GiB of HBM per device.

```python
import jax
import jax.numpy as jnp
from jax import lax

BATCH = 1
SEQ_LEN = 3072
D_MODEL = 5120
Q_HEADS = 40
KV_HEADS = 8
HEAD_DIM = 128
REF_ROWS = 128

CHUNK = 2 ** 13
ROPE_BASE = 500000.0
NORM_EPS = 1e-5
QK_EPS = 1e-6
TEMP_SCALE = 0.1
NEG_BIG = -1e30


def draw_positions(key):
    key_chunk, key_shift = jax.random.split(key)
    chunk_no = jax.random.randint(key_chunk, (), 2, 6)
    shift = jax.random.randint(key_shift, (), 1, min(SEQ_LEN, CHUNK))
    return (chunk_no * CHUNK - shift + jnp.arange(SEQ_LEN)).astype(jnp.int32)


def rope_tables(positions):
    half = HEAD_DIM // 2
    inv_freq = ROPE_BASE ** (-(jnp.arange(half).astype(jnp.float32) * 2.0 / HEAD_DIM))
    angles = positions.astype(jnp.float32)[:, None] * inv_freq[None, :]
    angles = jnp.concatenate([angles, angles], axis=1)
    return jnp.cos(angles), jnp.sin(angles)


def setup_inputs(seed: int = 0) -> dict:
    keys = jax.random.split(jax.random.key(seed), 16)
    positions = draw_positions(keys[0])
    rope_cos, rope_sin = rope_tables(positions)
    q_width = Q_HEADS * HEAD_DIM
    kv_width = KV_HEADS * HEAD_DIM
    act_shape = (BATCH, SEQ_LEN, D_MODEL)

    def weight(sub_key, rows, cols):
        return (jax.random.normal(sub_key, (rows, cols), jnp.float32) * rows ** -0.5).astype(jnp.bfloat16)

    def gain(sub_key):
        return jax.random.uniform(sub_key, (D_MODEL,), jnp.float32, 0.5, 1.5).astype(jnp.bfloat16)

    return {
        'x_in': jax.random.normal(keys[1], act_shape, jnp.float32).astype(jnp.bfloat16),
        'positions': positions,
        'rope_cos': rope_cos,
        'rope_sin': rope_sin,
        'norm_a': gain(keys[3]),
        'wq_a': weight(keys[4], D_MODEL, q_width),
        'wk_a': weight(keys[5], D_MODEL, kv_width),
        'wv_a': weight(keys[6], D_MODEL, kv_width),
        'wo_a': weight(keys[7], q_width, D_MODEL),
        'norm_b': gain(keys[8]),
        'wq_b': weight(keys[9], D_MODEL, q_width),
        'wk_b': weight(keys[10], D_MODEL, kv_width),
        'wv_b': weight(keys[11], D_MODEL, kv_width),
        'wo_b': weight(keys[12], q_width, D_MODEL),
        'grad_y': jax.random.normal(keys[2], act_shape, jnp.float32).astype(jnp.bfloat16),
    }


def rms_norm(act, gamma):
    act_wide = act.astype(jnp.float32)
    inv_rms = lax.rsqrt(jnp.mean(act_wide * act_wide, axis=-1, keepdims=True) + NORM_EPS)
    return (act_wide * inv_rms * gamma.astype(jnp.float32)).astype(jnp.bfloat16)


def project(act, weight):
    rows = act.shape[0] * act.shape[1]
    flat = jnp.dot(act.reshape(rows, act.shape[2]), weight, preferred_element_type=jnp.float32)
    return flat.reshape(act.shape[0], act.shape[1], weight.shape[1]).astype(jnp.bfloat16)


def rotate(wide, cos_tab, sin_tab):
    half = HEAD_DIM // 2
    turned = jnp.concatenate([-wide[..., half:], wide[..., :half]], axis=-1)
    return wide * cos_tab[None, :, None, :] + turned * sin_tab[None, :, None, :]


def qk_prep(raw_val, cos_tab, sin_tab):
    wide = rotate(raw_val.astype(jnp.float32), cos_tab, sin_tab)
    return (wide * lax.rsqrt(jnp.mean(wide * wide, axis=-1, keepdims=True) + QK_EPS)).astype(jnp.bfloat16)


def temperature(positions):
    return jnp.log(((positions + 1) // CHUNK).astype(jnp.float32) + 1.0) * TEMP_SCALE + 1.0


def attention(queries, keys, values, positions, local):
    scale = HEAD_DIM ** -0.5
    groups = Q_HEADS // KV_HEADS
    n_blocks = SEQ_LEN // REF_ROWS

    def block_attend(q_rows, q_pos, keys_wide, vals_wide, key_pos):
        scores = jnp.einsum('bqkgd,bskd->bkgqs', q_rows.astype(jnp.float32), keys_wide) * scale
        allowed = key_pos[None, :] <= q_pos[:, None]
        if local:
            allowed = jnp.logical_and(allowed, (key_pos // CHUNK)[None, :] == (q_pos // CHUNK)[:, None])
        attn_prob = jax.nn.softmax(jnp.where(allowed, scores, NEG_BIG), axis=-1).astype(jnp.bfloat16)
        attn_out = jnp.einsum('bkgqs,bskd->bqkgd', attn_prob.astype(jnp.float32), vals_wide)
        return attn_out.astype(jnp.bfloat16)

    keys_wide = keys.astype(jnp.float32)
    vals_wide = values.astype(jnp.float32)
    attend = jax.checkpoint(block_attend)

    def one_block(block_in):
        return attend(block_in[0], block_in[1], keys_wide, vals_wide, positions)

    q_blocks = jnp.moveaxis(queries.reshape(BATCH, n_blocks, REF_ROWS, KV_HEADS, groups, HEAD_DIM), 1, 0)
    block_outs = lax.map(one_block, (q_blocks, positions.reshape(n_blocks, REF_ROWS)))
    return jnp.moveaxis(block_outs, 0, 1).reshape(BATCH, SEQ_LEN, Q_HEADS * HEAD_DIM)


def forward(x_in, positions, rope_cos, rope_sin, norm_a, wq_a, wk_a, wv_a, wo_a, norm_b, wq_b, wk_b, wv_b, wo_b):
    q_shape = (BATCH, SEQ_LEN, KV_HEADS, Q_HEADS // KV_HEADS, HEAD_DIM)
    kv_shape = (BATCH, SEQ_LEN, KV_HEADS, HEAD_DIM)
    xn_a = rms_norm(x_in, norm_a)
    query_a = qk_prep(project(xn_a, wq_a).reshape(BATCH, SEQ_LEN, Q_HEADS, HEAD_DIM), rope_cos, rope_sin).reshape(q_shape)
    key_a = qk_prep(project(xn_a, wk_a).reshape(kv_shape), rope_cos, rope_sin)
    value_a = project(xn_a, wv_a).reshape(kv_shape)
    out_a = attention(query_a, key_a, value_a, positions, True)
    h_mid = (x_in.astype(jnp.float32) + project(out_a, wo_a).astype(jnp.float32)).astype(jnp.bfloat16)
    xn_b = rms_norm(h_mid, norm_b)
    q_temp = temperature(positions)[None, :, None]
    query_b = (project(xn_b, wq_b).astype(jnp.float32) * q_temp).astype(jnp.bfloat16).reshape(q_shape)
    key_b = project(xn_b, wk_b).reshape(kv_shape)
    value_b = project(xn_b, wv_b).reshape(kv_shape)
    out_b = attention(query_b, key_b, value_b, positions, False)
    return (h_mid.astype(jnp.float32) + project(out_b, wo_b).astype(jnp.float32)).astype(jnp.bfloat16)


def reference(x_in, positions, rope_cos, rope_sin, norm_a, wq_a, wk_a, wv_a, wo_a, norm_b, wq_b, wk_b, wv_b, wo_b, grad_y):
    def layers(x_arg, gain_a, w_qa, w_ka, w_va, w_oa, gain_b, w_qb, w_kb, w_vb, w_ob):
        return forward(x_arg, positions, rope_cos, rope_sin, gain_a, w_qa, w_ka, w_va, w_oa, gain_b, w_qb, w_kb, w_vb, w_ob)

    out_y, pullback = jax.vjp(layers, x_in, norm_a, wq_a, wk_a, wv_a, wo_a, norm_b, wq_b, wk_b, wv_b, wo_b)
    grads = pullback(grad_y)
    return (out_y, grads[0], grads[1], grads[2], grads[3], grads[4], grads[5], grads[6], grads[7], grads[8], grads[9], grads[10])
```

```python
import functools
import jax
import jax.numpy as jnp
from jax import lax
from jax.experimental import pallas as pl
from jax.experimental.pallas import tpu as pltpu
from jax.sharding import PartitionSpec as P

CHUNK = 8192
NORM_EPS = 1e-5
QK_EPS = 1e-6
TEMP_SCALE = 0.1
NEG_BIG = -1e30
JOIN = 8
LOG2E = 1.4426950408889634


def rms_norm(act, gamma):
    act_wide = act.astype(jnp.float32)
    inv_rms = lax.rsqrt(jnp.mean(act_wide * act_wide, axis=-1, keepdims=True) + NORM_EPS)
    return (act_wide * inv_rms * gamma.astype(jnp.float32)).astype(jnp.bfloat16)


def norm_backward(act, gamma, grad_out):
    act_wide = act.astype(jnp.float32)
    inv_rms = lax.rsqrt(jnp.mean(act_wide * act_wide, axis=-1, keepdims=True) + NORM_EPS)
    x_hat = act_wide * inv_rms
    grad_hat = grad_out * gamma.astype(jnp.float32)
    return inv_rms * (grad_hat - x_hat * jnp.mean(grad_hat * x_hat, axis=-1, keepdims=True))


def rotate(wide, cos_tab, sin_tab):
    half = wide.shape[-1] // 2
    turned = jnp.concatenate([-wide[..., half:], wide[..., :half]], axis=-1)
    return wide * cos_tab[:, None, :] + turned * sin_tab[:, None, :]


def qk_prep(raw_val, cos_tab, sin_tab):
    wide = rotate(raw_val.astype(jnp.float32), cos_tab, sin_tab)
    return (wide * lax.rsqrt(jnp.mean(wide * wide, axis=-1, keepdims=True) + QK_EPS)).astype(jnp.bfloat16)


def temperature(positions):
    return jnp.log(((positions + 1) // CHUNK).astype(jnp.float32) + 1.0) * TEMP_SCALE + 1.0


def dot(lhs, rhs, lhs_dim, rhs_dim):
    return lax.dot_general(lhs, rhs, (((lhs_dim,), (rhs_dim,)), ((), ())), preferred_element_type=jnp.float32)


def masked_scores(raw, first_key, first_query, cut):
    key_at = first_key + lax.broadcasted_iota(jnp.int32, raw.shape, 0)
    query_at = first_query + lax.broadcasted_iota(jnp.int32, (1, raw.shape[1]), 1)
    lowest = jnp.where(query_at >= cut, cut, 0)
    return jnp.where((key_at <= query_at) & (key_at >= lowest), raw, NEG_BIG)


def attn_fwd_kernel(local, coef, info, q_ref, k_ref, v_ref, o_ref, lse_ref, score):
    rank, cut = info[0], info[1]
    block, width = q_ref.shape
    queries = q_ref[...]
    span = score.shape[2]
    n_lane = span // width
    last = rank // (span // block)

    def rows(step):
        return pl.ds(pl.multiple_of(step * span, span), span)

    def raw_step(step, carry, masked):
        top, total = carry
        raw = dot(queries, k_ref[rows(step), :], 1, 1)
        if masked:
            query_at = rank * block + lax.broadcasted_iota(jnp.int32, (block, 1), 0)
            key_at = step * span + lax.broadcasted_iota(jnp.int32, raw.shape, 1)
            lowest = jnp.where(query_at >= cut, cut, 0)
            raw = jnp.where((key_at <= query_at) & (key_at >= lowest), raw, NEG_BIG)
        score[step] = raw
        parts = [raw[:, at * width:(at + 1) * width] * coef for at in range(n_lane)]
        higher = functools.reduce(jnp.maximum, parts, top)
        total = total * jnp.exp2(top - higher)
        for part in parts:
            total += jnp.exp2(part - higher)
        return higher, total

    carry = (jnp.full((block, width), NEG_BIG, jnp.float32), jnp.zeros((block, width), jnp.float32))
    carry = lax.fori_loop(0, last, lambda s, c: raw_step(s, c, local), carry)
    lane_top, lane_total = raw_step(last, carry, True)
    top = jnp.max(lane_top, axis=1, keepdims=True)
    total = jnp.sum(lane_total * jnp.exp2(lane_top - top), axis=1, keepdims=True)
    lse = top + jnp.log2(total)

    def out_step(step, acc):
        prob = jnp.exp2(score[step] * coef - lse).astype(jnp.bfloat16)
        return acc + dot(prob, v_ref[rows(step), :], 1, 0)

    acc = lax.fori_loop(0, last + 1, out_step, jnp.zeros((block, width), jnp.float32))
    o_ref[...] = acc.astype(jnp.bfloat16)
    lse_ref[0] = jnp.broadcast_to(lse, (block, width)).T[:1]


def attn_bwd_kernel(local, coef, scale, groups, info, q_ref, k_ref, v_ref, o_ref, do_ref, lse_ref,
                    dq_ref, dkv_ref, dk_acc, dv_acc):
    head = pl.program_id(0)
    group = lax.rem(head, groups)
    rank, cut = info[0], info[1]
    block, width = q_ref.shape
    span = JOIN * block
    last = rank // JOIN
    queries = q_ref[...]
    grads = do_ref[...]
    lse = lse_ref[0]
    delta = jnp.sum((grads.astype(jnp.float32) * o_ref[...].astype(jnp.float32)).T, axis=0, keepdims=True)

    @pl.when(group == 0)
    def _():
        dk_acc[...] = jnp.zeros_like(dk_acc)
        dv_acc[...] = jnp.zeros_like(dv_acc)

    def step_fn(step, acc, masked):
        where = pl.ds(pl.multiple_of(step * span, span), span)
        keys = k_ref[where, :]
        raw = dot(keys, queries, 1, 1)
        if masked:
            raw = masked_scores(raw, step * span, rank * block, cut)
        prob = jnp.exp2(raw * coef - lse)
        dprob = dot(v_ref[where, :], grads, 1, 1)
        dscore = (prob * (dprob - delta) * scale).astype(jnp.bfloat16)
        dv_acc[where, :] += dot(prob.astype(jnp.bfloat16), grads, 1, 0)
        dk_acc[where, :] += dot(dscore, queries, 1, 0)
        return acc + dot(keys, dscore, 0, 0)

    acc = lax.fori_loop(0, last, lambda s, a: step_fn(s, a, local), jnp.zeros((width, block), jnp.float32))
    acc = step_fn(last, acc, True)
    dq_ref[...] = acc.T.astype(dq_ref.dtype)
    kv_local = dkv_ref.shape[1] // (2 * width)
    for kv in range(kv_local):
        @pl.when(head == kv * groups + groups - 1)
        def _():
            dkv_ref[:, kv * width:(kv + 1) * width] = dk_acc[...].astype(jnp.bfloat16)
            dkv_ref[:, (kv_local + kv) * width:(kv_local + kv + 1) * width] = dv_acc[...].astype(jnp.bfloat16)


def attn_specs(seq_len, block, width, kv_local, groups):
    return [pl.BlockSpec((block, width), lambda h, info: (0, h)),
            pl.BlockSpec((seq_len, width), lambda h, info: (0, h // groups)),
            pl.BlockSpec((seq_len, width), lambda h, info: (0, kv_local + h // groups))]


def attn_forward(local, info, query, kv_all, width):
    block, seq_len = query.shape[0], kv_all.shape[0]
    heads, kv_local = query.shape[1] // width, kv_all.shape[1] // (2 * width)
    groups = heads // kv_local
    scale = width ** -0.5
    flops = 4 * heads * block * seq_len * width
    return pl.pallas_call(
        functools.partial(attn_fwd_kernel, local, scale * LOG2E),
        out_shape=(jax.ShapeDtypeStruct(query.shape, jnp.bfloat16), jax.ShapeDtypeStruct((heads, 1, block), jnp.float32)),
        grid_spec=pltpu.PrefetchScalarGridSpec(
            num_scalar_prefetch=1, grid=(heads,),
            in_specs=attn_specs(seq_len, block, width, kv_local, groups),
            out_specs=[pl.BlockSpec((block, width), lambda h, info: (0, h)),
                       pl.BlockSpec((1, 1, block), lambda h, info: (h, 0, 0))],
            scratch_shapes=[pltpu.VMEM((seq_len // (JOIN * block), block, JOIN * block), jnp.float32)]),
        compiler_params=pltpu.CompilerParams(vmem_limit_bytes=40 * 2 ** 20),
        cost_estimate=pl.CostEstimate(flops=flops * 4, bytes_accessed=8 * 2 ** 20, transcendentals=0),
        name='attn_fwd_a' if local else 'attn_fwd_b',
    )(info, query, kv_all, kv_all)


def attn_backward(local, info, query, kv_all, out, grad_out, lse, width, dq_dtype):
    block, seq_len = query.shape[0], kv_all.shape[0]
    heads, kv_local = query.shape[1] // width, kv_all.shape[1] // (2 * width)
    groups = heads // kv_local
    scale = width ** -0.5
    flops = 10 * heads * block * seq_len * width
    head_spec = pl.BlockSpec((block, width), lambda h, info: (0, h))
    return pl.pallas_call(
        functools.partial(attn_bwd_kernel, local, scale * LOG2E, scale, groups),
        out_shape=(jax.ShapeDtypeStruct(query.shape, dq_dtype), jax.ShapeDtypeStruct(kv_all.shape, jnp.bfloat16)),
        grid_spec=pltpu.PrefetchScalarGridSpec(
            num_scalar_prefetch=1, grid=(heads,),
            in_specs=attn_specs(seq_len, block, width, kv_local, groups)
            + [head_spec, head_spec, pl.BlockSpec((1, 1, block), lambda h, info: (h, 0, 0))],
            out_specs=[head_spec, pl.BlockSpec(kv_all.shape, lambda h, info: (0, 0))],
            scratch_shapes=[pltpu.VMEM((seq_len, width), jnp.float32), pltpu.VMEM((seq_len, width), jnp.float32)]),
        compiler_params=pltpu.CompilerParams(vmem_limit_bytes=40 * 2 ** 20),
        cost_estimate=pl.CostEstimate(flops=flops * 4, bytes_accessed=12 * 2 ** 20, transcendentals=0),
        name='attn_bwd_a' if local else 'attn_bwd_b',
    )(info, query, kv_all, kv_all, out, grad_out, lse)


def wgrad_kernel(n_blocks, flip, *refs):
    acts, grads = refs[:n_blocks], refs[n_blocks:2 * n_blocks]
    out_ref, turned = refs[2 * n_blocks], refs[2 * n_blocks + 1]
    block = acts[0].shape[0]

    @pl.when(pl.program_id(0) == 0)
    def _():
        for at, act in enumerate(acts):
            turned[:, at * block:(at + 1) * block] = act[...].T

    acc = dot(turned[:, :block], grads[0][...], 1, 0)
    for at in range(1, n_blocks):
        acc += dot(turned[:, at * block:(at + 1) * block], grads[at][...], 1, 0)
    out_ref[...] = (acc.T if flip else acc).astype(jnp.bfloat16)


def weight_grad(acts, grads, flip=False):
    n_blocks = len(acts)
    block, rows = acts[0].shape
    cols = grads[0].shape[1]
    tile = 256
    return pl.pallas_call(
        functools.partial(wgrad_kernel, n_blocks, flip),
        out_shape=jax.ShapeDtypeStruct((cols, rows) if flip else (rows, cols), jnp.bfloat16),
        grid=(cols // tile,),
        in_specs=[pl.BlockSpec((block, rows), lambda j: (0, 0))] * n_blocks
        + [pl.BlockSpec((block, tile), lambda j: (0, j))] * n_blocks,
        out_specs=pl.BlockSpec((tile, rows), lambda j: (j, 0)) if flip else pl.BlockSpec((rows, tile), lambda j: (0, j)),
        scratch_shapes=[pltpu.VMEM((rows, n_blocks * block), jnp.bfloat16)],
        compiler_params=pltpu.CompilerParams(vmem_limit_bytes=48 * 2 ** 20),
        cost_estimate=pl.CostEstimate(flops=2 * n_blocks * block * rows * cols, bytes_accessed=16 * 2 ** 20, transcendentals=0),
    )(*acts, *grads)


def solution(mesh):
    cp_size = mesh.shape['cp']
    row_spec = P(None, 'cp', None)
    col_spec = P(None, 'tp')
    grid_spec = P('cp', 'tp')
    out_rows = P(('tp', 'cp'), None)
    in_specs = (row_spec, P('cp'), P('cp', None), P('cp', None),
                P(None), col_spec, col_spec, col_spec, P('tp', None),
                P(None), col_spec, col_spec, col_spec, P('tp', None), row_spec)
    out_specs = (row_spec, row_spec,
                 P('cp'), grid_spec, grid_spec, grid_spec, out_rows,
                 P('cp'), grid_spec, grid_spec, grid_spec, out_rows)

    def swap(val, mask):
        return lax.ppermute(val, 'cp', [(source, source ^ mask) for source in range(cp_size)])

    def gather_xor(val):
        near = [val] + [swap(val, mask) for mask in range(2, cp_size, 2)]
        return near + [swap(part, 1) for part in near]

    order = list(range(0, cp_size, 2)) + [mask ^ 1 for mask in range(0, cp_size, 2)]

    def exchange_cols(val):
        cols = val.shape[1] // cp_size
        rank = lax.axis_index('cp')
        return [(lambda piece: piece if mask == 0 else swap(piece, mask))(
            lax.dynamic_slice_in_dim(val, (rank ^ mask) * cols, cols, axis=1)) for mask in order]

    def gain_grad(act, partial):
        act_wide = act.astype(jnp.float32)
        inv_rms = lax.rsqrt(jnp.mean(act_wide * act_wide, axis=-1, keepdims=True) + NORM_EPS)
        total = jnp.sum(partial.astype(jnp.float32) * (act_wide * inv_rms), axis=0)
        rank = lax.axis_index('cp')
        mask = cp_size // 2
        while mask:
            rows = total.shape[0] // 2
            upper = (rank // mask) % 2
            theirs = swap(lax.dynamic_slice_in_dim(total, (1 - upper) * rows, rows), mask)
            total = lax.dynamic_slice_in_dim(total, upper * rows, rows) + theirs
            mask //= 2
        mask = 1
        while mask < mesh.shape['tp']:
            total = total + lax.ppermute(total, 'tp', [(source, source ^ mask) for source in range(mesh.shape['tp'])])
            mask *= 2
        return total.astype(jnp.bfloat16)

    def exchange_rows(val):
        return lax.all_to_all(val, 'cp', split_axis=0, concat_axis=1, tiled=True)

    def body(x_in, positions, rope_cos, rope_sin, norm_a, wq_a, wk_a, wv_a, wo_a,
             norm_b, wq_b, wk_b, wv_b, wo_b, grad_y):
        x_in, grad_y = x_in[0], grad_y[0]
        block = x_in.shape[0]
        width = rope_cos.shape[1]
        kv_local = wk_a.shape[1] // width
        kv_cols = kv_local * width
        cp_rank = lax.axis_index('cp')
        first = positions[0] - cp_rank * block
        info_a = jnp.stack([cp_rank, lax.rem(CHUNK - lax.rem(first, CHUNK), CHUNK)]).astype(jnp.int32)
        info_b = jnp.stack([cp_rank, jnp.zeros_like(cp_rank)]).astype(jnp.int32)
        q_temp = temperature(positions)[:, None]

        def prep(raw_val):
            heads = raw_val.reshape(block, -1, width)
            return qk_prep(heads, rope_cos, rope_sin).reshape(raw_val.shape)

        def project(act, weight):
            return dot(act, weight, 1, 0).astype(jnp.bfloat16)

        def gather_kv(key, value):
            return lax.all_gather(jnp.concatenate([key, value], axis=1), 'cp', axis=0, tiled=True)

        def scatter_kv(grad):
            return lax.psum_scatter(grad, 'cp', scatter_dimension=0, tiled=True)

        grad_y_cols = exchange_cols(grad_y)
        xn_a = rms_norm(x_in, norm_a)
        key_a, k_pull = jax.vjp(prep, project(xn_a, wk_a))
        kv_a = gather_kv(key_a, project(xn_a, wv_a))
        query_a, q_pull = jax.vjp(prep, project(xn_a, wq_a))
        xn_a_cols = exchange_cols(xn_a)
        out_a, lse_a = attn_forward(True, info_a, query_a, kv_a, width)
        attn_a = lax.psum(project(out_a, wo_a), 'tp')
        out_a_all = gather_xor(out_a)
        grad_ob = dot(grad_y, wo_b, 1, 1).astype(jnp.bfloat16)
        attn_a, grad_ob, grad_y_cols, xn_a_cols, out_a_all = lax.optimization_barrier(
            (attn_a, grad_ob, grad_y_cols, xn_a_cols, out_a_all))
        h_mid = (x_in.astype(jnp.float32) + attn_a.astype(jnp.float32)).astype(jnp.bfloat16)

        xn_b = rms_norm(h_mid, norm_b)
        kv_b = gather_kv(project(xn_b, wk_b), project(xn_b, wv_b))
        query_b = (project(xn_b, wq_b).astype(jnp.float32) * q_temp).astype(jnp.bfloat16)
        kv_b, xn_b_late = lax.optimization_barrier((kv_b, xn_b))
        xn_b_cols = exchange_cols(xn_b_late)
        out_b, lse_b = attn_forward(False, info_b, query_b, kv_b, width)
        attn_b = project(out_b, wo_b)
        attn_b, lse_b, xn_b_cols = lax.optimization_barrier((attn_b, lse_b, xn_b_cols))
        half = block // 2
        attn_b_lo = lax.psum(attn_b[:half], 'tp')
        out_b_all = gather_xor(out_b)

        grad_q_b, grad_kv_b = attn_backward(False, info_b, query_b, kv_b, out_b, grad_ob, lse_b, width, jnp.float32)
        grad_kv_b, attn_b_lo = lax.optimization_barrier((grad_kv_b, attn_b_lo))
        grad_kv_b = scatter_kv(grad_kv_b)
        grad_q_b = (grad_q_b * q_temp).astype(jnp.bfloat16)
        grad_q_b_all, grad_kv_b_all = gather_xor(grad_q_b), gather_xor(grad_kv_b)
        grad_xn_b = dot(grad_q_b, wq_b, 1, 1) + dot(grad_kv_b[:, :kv_cols], wk_b, 1, 1) + dot(grad_kv_b[:, kv_cols:], wv_b, 1, 1)
        grad_xn_b = grad_xn_b.astype(jnp.bfloat16)
        grad_norm_b = gain_grad(h_mid, grad_xn_b)
        grad_xn_b = lax.psum(grad_xn_b, 'tp')
        grad_wo_b = weight_grad(grad_y_cols, out_b_all, True)
        grad_wq_b = weight_grad(xn_b_cols, grad_q_b_all)
        grad_wkv_b = weight_grad(xn_b_cols, grad_kv_b_all)
        grad_xn_b, grad_wo_b, grad_wq_b, grad_wkv_b, grad_norm_b, attn_b = lax.optimization_barrier(
            (grad_xn_b, grad_wo_b, grad_wq_b, grad_wkv_b, grad_norm_b, attn_b))
        attn_b_hi = lax.psum(attn_b[half:], 'tp')
        grad_h = (grad_y.astype(jnp.float32) + norm_backward(h_mid, norm_b, grad_xn_b.astype(jnp.float32))).astype(jnp.bfloat16)

        grad_h_cols = exchange_cols(grad_h)
        grad_oa = dot(grad_h, wo_a, 1, 1).astype(jnp.bfloat16)
        grad_q_a, grad_kv_a = attn_backward(True, info_a, query_a, kv_a, out_a, grad_oa, lse_a, width, jnp.bfloat16)
        grad_kv_a, attn_b_hi, grad_h_cols = lax.optimization_barrier((grad_kv_a, attn_b_hi, grad_h_cols))
        attn_b = jnp.concatenate([attn_b_lo, attn_b_hi], axis=0)
        out_y = (h_mid.astype(jnp.float32) + attn_b.astype(jnp.float32)).astype(jnp.bfloat16)
        grad_kv_a = scatter_kv(grad_kv_a)
        grad_q_a = q_pull(grad_q_a)[0]
        grad_kv_a, grad_q_a_late, grad_wo_b = lax.optimization_barrier((grad_kv_a, grad_q_a, grad_wo_b))
        grad_q_a_all = gather_xor(grad_q_a_late)
        grad_wo_b = exchange_rows(grad_wo_b)
        grad_k_a = k_pull(grad_kv_a[:, :kv_cols])[0]
        grad_v_a = grad_kv_a[:, kv_cols:]
        grad_kv_a_all = gather_xor(jnp.concatenate([grad_k_a, grad_v_a], axis=1))
        grad_xn_a = dot(grad_q_a, wq_a, 1, 1) + dot(grad_k_a, wk_a, 1, 1) + dot(grad_v_a, wv_a, 1, 1)
        grad_xn_a = grad_xn_a.astype(jnp.bfloat16)
        grad_norm_a = gain_grad(x_in, grad_xn_a)
        grad_xn_a = lax.psum(grad_xn_a, 'tp')
        grad_wo_a = exchange_rows(weight_grad(grad_h_cols, out_a_all, True))
        grad_wq_a = weight_grad(xn_a_cols, grad_q_a_all)
        grad_wkv_a = weight_grad(xn_a_cols, grad_kv_a_all)
        grad_xn_a, grad_wo_a, grad_wq_a, grad_wkv_a, grad_norm_a, grad_wo_b, out_y = lax.optimization_barrier(
            (grad_xn_a, grad_wo_a, grad_wq_a, grad_wkv_a, grad_norm_a, grad_wo_b, out_y))
        grad_x = (grad_h.astype(jnp.float32) + norm_backward(x_in, norm_a, grad_xn_a.astype(jnp.float32))).astype(jnp.bfloat16)

        return (out_y[None], grad_x[None],
                grad_norm_a, grad_wq_a, grad_wkv_a[:, :kv_cols], grad_wkv_a[:, kv_cols:], grad_wo_a,
                grad_norm_b, grad_wq_b, grad_wkv_b[:, :kv_cols], grad_wkv_b[:, kv_cols:], grad_wo_b)

    return jax.shard_map(body, mesh=mesh, in_specs=in_specs, out_specs=out_specs, check_vma=False)
```
